32 devices in a mesh: dp: 8 (over y, x, core), expert: 4 (over z).
Axes of the slice: x: 2, y: 2, z: 4, core: 2. Of those that a mesh axis runs over, the one named last changes fastest.
Arguments:
- tokens: bfloat16 [4096, 2048], P(('dp', 'expert')), may hold values from -6 to 6
- out_grad: bfloat16 [4096, 2048], P(('dp', 'expert')), may hold values from -6 to 6
- gate_prob: float32 [4096, 1], P(('dp', 'expert')), may hold values from 0.2 to 1
- routing: int32 [4096, 1], P(('dp', 'expert')), may hold values from 0 to 3; in each aligned block of 128 rows (0 to 127, 128 to 255, ...) at most 64 rows name the same one
- expert_weights: bfloat16 [4, 2048, 1152], P('expert'), may hold values from -0.125 to 0.125
Outputs:
- input_grad: bfloat16 [4096, 2048], P(('dp', 'expert'))
- weight_grad: float32 [4, 2048, 1152], P('expert', 'dp')
The draws below stay inside these ranges and needn't reach their ends.
Inputs may be any that keep to these rules, and one draw needn't show every extreme that they name: `routing`: among the tokens of one device at most 64 go to any one expert; in some devices' tokens an expert gets exactly 64.
All inputs are finite; a program needn't handle non-finite values.
Results may differ from the reference program's by a relative error of at most 0.014.
Values may be sent and summed in bfloat16 or wider, within the bound.
No kernel may reach another device: no remote copies, remote signals or barrier semaphores. Data moves between devices by JAX's collectives and lax.ppermute only.
A program may use at most 64 MiB of HBM per device.

```python
import math
from functools import partial
import jax
import jax.numpy as jnp
import numpy as np
from jax import lax

D = 2048
FF = 384
TOK_DEV = 128
TOKENS = 4096
EXPERTS_TURN = 4
CAP = 64
GROUP_ROWS = 1024
N_DP = 8
N_EXPERT = 4


def block_levels(key, shape, shards, smallest, high):
    level, own = 1.0, jax.random.fold_in(key, 6)
    for axis_at, shards_of in shards:
        heights = jnp.exp(jax.random.uniform(jax.random.fold_in(own, axis_at), (shards_of,), jnp.float32, smallest / len(shards), high / len(shards)))
        level = level * jnp.repeat(heights, shape[axis_at] // shards_of).reshape([-1 if axis == axis_at else 1 for axis in range(len(shape))])
    return level


def shared_out(stream_key, own, number, rows, number_of, top, most, slope):
    order = jax.random.permutation(stream_key, number_of)
    heavy_load, common = shares(number_of, rows * top, most, slope, True), shares(number_of, rows * top, most, slope, False)
    places = jnp.arange(number_of)

    def named(sizes, rotation):
        used = int((sizes > 0).sum())
        fixed = max(1, used // 4)
        moved = fixed + (places - fixed + rotation * (used - fixed)) % max(1, number_of - fixed)
        return jnp.zeros((number_of,), jnp.int32).at[order[jnp.where(places < fixed, places, moved)]].set(jnp.asarray(sizes, jnp.int32))

    sizes = jnp.where(number % 4 == 0, named(heavy_load, number // 4), named(common, number - number // 4 - 1))
    mixed = jax.random.permutation(jax.random.fold_in(own, 3), number_of)
    giver, receiver = mixed[0:number_of // 2 * 2:2], mixed[1:number_of // 2 * 2:2]
    slack = jnp.minimum(sizes[giver] - 1, most - sizes[receiver]) // 2
    slack = jnp.where((giver == order[0]) | (receiver == order[0]) | (sizes[receiver] == 0), 0, jnp.maximum(slack, 0))
    moved = jax.random.randint(jax.random.fold_in(own, 4), (number_of // 2,), 0, 1 << 20) % (slack + 1)
    sizes = sizes.at[giver].add(-moved).at[receiver].add(moved)
    labels = jnp.searchsorted(jnp.cumsum(sizes), jnp.arange(rows * top), side="right").astype(jnp.int32)
    grid = labels.reshape(top, rows).T
    grid = grid[jax.random.permutation(jax.random.fold_in(own, 1), rows)]
    rotation = jax.random.randint(jax.random.fold_in(own, 2), (rows, 1), 0, top)
    return jnp.take_along_axis(grid, (jnp.arange(top)[None, :] + rotation) % top, axis=1)


def shares(number_of, total, reach, slope, full):
    loads = [(1 << 20) // math.isqrt(standing ** slope) + 1 for standing in range(1, number_of + 1)]
    largest = reach if full else min(reach, max(-(-total // number_of), total * loads[0] // sum(loads)))
    least = 1 if total - largest >= number_of - 1 else 0
    counts, rest = [largest] + [least] * (number_of - 1), total - largest - least * (number_of - 1)
    while rest > 0:
        candidates = [i for i in range(1, number_of) if counts[i] < largest] or [i for i in range(1, number_of) if counts[i] < reach]
        whole, left = sum([loads[i] for i in candidates]), rest
        for i in candidates:
            more = min(reach - counts[i], max(1, left * loads[i] // whole), rest)
            counts[i] = counts[i] + more
            rest = rest - more
    return np.array(counts)


def noise(rng, extent, width, reach, pieces=(), kind=jnp.bfloat16):
    drawn = jax.random.normal(rng, extent, jnp.float32) * width
    if len(pieces) > 0:
        drawn = block_levels(rng, extent, pieces, -0.22, 0.18) * drawn
    return jnp.clip(drawn, min=-reach, max=reach).astype(kind)


def setup_inputs(seed: int = 0) -> dict:
    streams_of = jax.random.split(jax.random.key(seed), 6)
    tokens = noise(streams_of[0], (TOKENS, D), 1.0, 6.0, ((0, 32),))
    out_grad = noise(streams_of[1], (TOKENS, D), 1.0, 6.0, ((0, 32),))
    gate_prob = jnp.clip(0.2 + 0.8 * jax.random.uniform(streams_of[2], (TOKENS, 1), jnp.float32) ** block_levels(streams_of[2], (TOKENS, 1), ((0, 32),), -0.2, 0.2), 0.2, 1.0)
    routing_keys = jax.random.split(jax.random.fold_in(streams_of[3], 1), TOKENS // TOK_DEV)
    routing_turns = jax.random.permutation(jax.random.fold_in(streams_of[3], 3), TOKENS // TOK_DEV)
    routing = jax.vmap(lambda own, number: shared_out(jax.random.fold_in(streams_of[3], 2), own, number, TOK_DEV, N_EXPERT, 1, CAP, 2))(routing_keys, routing_turns).reshape((TOKENS, 1))
    expert_weights = noise(streams_of[4], (EXPERTS_TURN, D, 3 * FF), D ** -0.5, 0.125, ((0, 4),))
    return {"tokens": tokens, "out_grad": out_grad, "gate_prob": gate_prob, "routing": routing, "expert_weights": expert_weights}


def slot_of(route_block, capacity, experts):
    onehot = (route_block[:, None] == jnp.arange(experts, dtype=jnp.int32)[None, :]).astype(jnp.int32)
    before = jnp.cumsum(onehot, axis=0) - onehot
    position = jnp.sum(before * onehot, axis=1).astype(jnp.int32)
    return (route_block * capacity + position).astype(jnp.int32)


def expert_rows(weights, rows_in, grad_in):
    hidden_width = weights.shape[1] // 3
    pair_weights = weights[:, :2 * hidden_width]
    down_weights = weights[:, 2 * hidden_width:]
    pre_act = jnp.dot(rows_in, pair_weights, preferred_element_type=jnp.float32)
    pre_gate = pre_act[:, :hidden_width]
    pre_up = pre_act[:, hidden_width:]
    sigmoid_gate = jax.nn.sigmoid(pre_gate)
    active = pre_gate * sigmoid_gate
    hidden = (active * pre_up).astype(jnp.bfloat16)
    grad_hidden = jnp.dot(grad_in, down_weights, preferred_element_type=jnp.float32)
    grad_gate = grad_hidden * pre_up * (sigmoid_gate * (1.0 + pre_gate * (1.0 - sigmoid_gate)))
    grad_up = grad_hidden * active
    grad_pair = jnp.concatenate([grad_gate.astype(jnp.bfloat16), grad_up.astype(jnp.bfloat16)], axis=1)
    returned = lax.dot_general(grad_pair, pair_weights, (((1,), (1,)), ((), ())), preferred_element_type=jnp.float32)
    return returned.astype(jnp.bfloat16), hidden, grad_pair


def weight_term(rows_in, grad_in, hidden, grad_pair, grad_scale):
    contract = (((0,), (0,)), ((), ()))
    first_part = lax.dot_general(rows_in, grad_pair, contract, preferred_element_type=jnp.float32)
    second = lax.dot_general(grad_in, hidden, contract, preferred_element_type=jnp.float32)
    return grad_scale * jnp.concatenate([first_part, second], axis=1)


def reference(tokens, out_grad, gate_prob, routing, expert_weights):
    model_width = tokens.shape[1]
    grad_scale = float(GROUP_ROWS) ** -0.5
    scaled = (gate_prob * out_grad.astype(jnp.float32)).astype(jnp.bfloat16)
    tok_x = tokens.reshape(N_DP, N_EXPERT, TOK_DEV, model_width)
    tok_g = scaled.reshape(N_DP, N_EXPERT, TOK_DEV, model_width)
    routes = routing.reshape(N_DP, N_EXPERT, TOK_DEV)
    slotter = jax.vmap(partial(slot_of, capacity=CAP, experts=N_EXPERT))

    def one_expert(operands):
        weights, rows_in, grad_in = operands
        returned, hidden, grad_pair = expert_rows(weights, rows_in, grad_in)
        rounded = weight_term(rows_in, grad_in, hidden, grad_pair, grad_scale).astype(jnp.bfloat16)
        rounded = lax.optimization_barrier(rounded)
        return returned, rounded.astype(jnp.float32)

    def replica(running, blocks):
        block_x, block_g, block_r = blocks
        slot_index = slotter(block_r)
        source = jnp.broadcast_to(jnp.arange(N_EXPERT, dtype=jnp.int32)[:, None], slot_index.shape)
        buf_x = jnp.zeros((N_EXPERT, N_EXPERT * CAP, model_width), jnp.bfloat16).at[source, slot_index].set(block_x)
        buf_g = jnp.zeros((N_EXPERT, N_EXPERT * CAP, model_width), jnp.bfloat16).at[source, slot_index].set(block_g)
        buf_x = buf_x.reshape(N_EXPERT, N_EXPERT, CAP, model_width).transpose(1, 0, 2, 3).reshape(N_EXPERT, N_EXPERT * CAP, model_width)
        buf_g = buf_g.reshape(N_EXPERT, N_EXPERT, CAP, model_width).transpose(1, 0, 2, 3).reshape(N_EXPERT, N_EXPERT * CAP, model_width)
        returned, terms = lax.map(one_expert, (expert_weights, buf_x, buf_g))
        returned = returned.reshape(N_EXPERT, N_EXPERT, CAP, model_width).transpose(1, 0, 2, 3).reshape(N_EXPERT, N_EXPERT * CAP, model_width)
        return running + terms, returned[source, slot_index]

    initial = jnp.zeros((N_EXPERT, model_width, expert_weights.shape[2]), jnp.float32)
    totals, input_grads = lax.scan(replica, initial, (tok_x, tok_g, routes))
    return input_grads.reshape(TOKENS, model_width), totals
```

```python
import jax
import jax.numpy as jnp
from jax import lax
from jax.sharding import PartitionSpec as P


ROWS = (((0,), (0,)), ((), ()))


def slot_of(route_block, me, capacity, experts):
    relative = jnp.where(route_block >= me, route_block - me, route_block - me + experts)
    onehot = (relative[:, None] == jnp.arange(experts, dtype=jnp.int32)[None, :]).astype(jnp.int32)
    before = jnp.cumsum(onehot, axis=0) - onehot
    position = jnp.sum(before * onehot, axis=1)
    return relative * capacity + position


def shift(value, distance, size):
    return lax.ppermute(value, "expert", [(j, (j + distance) % size) for j in range(size)])


def exchange(pieces, sign):
    size = len(pieces)
    moved = {0: pieces[0]}
    for distance in sorted(range(1, size), key=lambda s: -min(s, size - s)):
        moved[distance] = shift(pieces[distance], sign * distance, size)
    return [moved[s] for s in range(size)]


def swap(value, bit, size):
    return lax.ppermute(value, "dp", [(j, j ^ bit) for j in range(size)])


def matmul(a, b):
    return jnp.dot(a, b, preferred_element_type=jnp.float32)


def local(tokens, out_grad, gate_prob, routing, expert_weights):
    tok_dev, model_width = tokens.shape
    experts = lax.axis_size("expert")
    replicas = lax.axis_size("dp")
    chips = replicas // 2
    chip_bits = chips.bit_length() - 1
    capacity = 2 * tok_dev // experts
    share_rows = model_width // replicas
    half_rows = share_rows // 2
    grad_scale = float(tok_dev * replicas) ** (-0.5)
    weights = expert_weights[0]
    hidden_width = weights.shape[1] // 3
    pair_weights = weights[:, : 2 * hidden_width]
    down_weights = weights[:, 2 * hidden_width :]
    me = lax.axis_index("expert")
    replica = lax.axis_index("dp")
    core = replica % 2
    chip = replica // 2

    slot_index = slot_of(routing[:, 0], me, capacity, experts)
    table = (
        jnp.arange(experts * capacity, dtype=jnp.int32)[:, None] == slot_index[None, :]
    ).astype(jnp.bfloat16)

    def split(rows):
        return [rows[s * capacity : (s + 1) * capacity] for s in range(experts)]

    send_x = matmul(table, tokens).astype(jnp.bfloat16)
    recv_x = exchange(split(send_x), 1)
    scaled = (gate_prob * out_grad.astype(jnp.float32)).astype(jnp.bfloat16)
    send_g = matmul(table, scaled).astype(jnp.bfloat16)
    recv_g = exchange(split(send_g), 1)

    orders = [list(range(chip_bits)), list(range(chip_bits))[::-1]]
    sends = [[r for r in range(chips) if r >> order[0] & 1] for order in orders]
    keeps = [[r for r in range(chips) if not r >> order[0] & 1] for order in orders]
    layout = [(r, h) for h in (0, 1) for r in sends[h]] + [(r, h) for h in (0, 1) for r in keeps[h]]

    def bands(rows, side):
        return jnp.concatenate(
            [
                lax.dynamic_slice_in_dim(
                    rows, ((chip ^ r) * 2 + side) * share_rows + h * half_rows, half_rows, 1
                )
                for r, h in layout
            ],
            axis=1,
        )

    def both_cores(rows):
        other = swap(bands(rows, 1 - core), 1, replicas)
        return jnp.concatenate([bands(rows, core), other], axis=0)

    rows_in = jnp.concatenate(recv_x, axis=0)
    pre_act = matmul(rows_in, pair_weights)
    wide_x = both_cores(rows_in)
    pre_gate = pre_act[:, :hidden_width]
    pre_up = pre_act[:, hidden_width:]
    sigmoid_gate = jax.nn.sigmoid(pre_gate)
    active = pre_gate * sigmoid_gate
    hidden = (active * pre_up).astype(jnp.bfloat16)

    grad_in = jnp.concatenate(recv_g, axis=0)
    grad_hidden = matmul(grad_in, down_weights)
    grad_gate = grad_hidden * pre_up * (sigmoid_gate * (1.0 + pre_gate * (1.0 - sigmoid_gate)))
    grad_up = grad_hidden * active
    grad_pair = jnp.concatenate(
        [grad_gate.astype(jnp.bfloat16), grad_up.astype(jnp.bfloat16)], axis=1
    )
    returned = lax.dot_general(
        grad_pair, pair_weights, (((1,), (1,)), ((), ())), preferred_element_type=jnp.float32
    ).astype(jnp.bfloat16)
    arrived = exchange(split(returned), -1)

    wide_g = both_cores(grad_in)
    wide_hidden = jnp.concatenate([hidden, swap(hidden, 1, replicas)], axis=0)
    wide_pair = jnp.concatenate([grad_pair, swap(grad_pair, 1, replicas)], axis=0)

    group = (chips // 2) * half_rows

    def block(index):
        cut = slice(index * group, (index + 1) * group)
        first = lax.dot_general(wide_x[:, cut], wide_pair, ROWS, preferred_element_type=jnp.float32)
        second = lax.dot_general(
            wide_g[:, cut], wide_hidden, ROWS, preferred_element_type=jnp.float32
        )
        return (grad_scale * jnp.concatenate([first, second], axis=1)).reshape(
            chips // 2, half_rows, 3 * hidden_width
        )

    outgoing = [
        swap(block(h).astype(jnp.bfloat16), 2 << orders[h][0], replicas) for h in (0, 1)
    ]
    kept = [block(2 + h) for h in (0, 1)]
    totals = []
    for h in (0, 1):
        value = kept[h] + outgoing[h].astype(jnp.float32)
        members = keeps[h]
        for bit in orders[h][1:]:
            out = [i for i, r in enumerate(members) if r >> bit & 1]
            stay = [i for i, r in enumerate(members) if not r >> bit & 1]
            parcel = jnp.concatenate([value[i : i + 1] for i in out], axis=0).astype(jnp.bfloat16)
            came = swap(parcel, 2 << bit, replicas).astype(jnp.float32)
            value = jnp.concatenate([value[i : i + 1] for i in stay], axis=0) + came
            members = [members[i] for i in stay]
        totals.append(value[0])
    weight_grad = jnp.concatenate(totals, axis=0)

    input_grad = lax.dot_general(
        table, jnp.concatenate(arrived, axis=0), ROWS, preferred_element_type=jnp.float32
    ).astype(jnp.bfloat16)
    return (input_grad, weight_grad.reshape(1, share_rows, 3 * hidden_width))


def solution(mesh):
    in_specs = (
        P(("dp", "expert"), None),
        P(("dp", "expert"), None),
        P(("dp", "expert"), None),
        P(("dp", "expert"), None),
        P("expert", None, None),
    )
    out_specs = (P(("dp", "expert"), None), P("expert", "dp", None))
    return jax.shard_map(local, mesh=mesh, in_specs=in_specs, out_specs=out_specs, check_vma=False)
```

```python
import jax
import jax.numpy as jnp
from jax import lax
from jax.sharding import PartitionSpec as P


ROWS = (((0,), (0,)), ((), ()))


def slot_of(route_block, me, capacity, experts):
    relative = jnp.where(route_block >= me, route_block - me, route_block - me + experts)
    onehot = (relative[:, None] == jnp.arange(experts, dtype=jnp.int32)[None, :]).astype(jnp.int32)
    before = jnp.cumsum(onehot, axis=0) - onehot
    position = jnp.sum(before * onehot, axis=1)
    return relative * capacity + position


def shift(value, distance, size):
    return lax.ppermute(value, "expert", [(j, (j + distance) % size) for j in range(size)])


def exchange(pieces, sign):
    size = len(pieces)
    moved = {0: pieces[0]}
    for distance in sorted(range(1, size), key=lambda s: -min(s, size - s)):
        moved[distance] = shift(pieces[distance], sign * distance, size)
    return [moved[s] for s in range(size)]


def swap(value, bit, size):
    return lax.ppermute(value, "dp", [(j, j ^ bit) for j in range(size)])


def matmul(a, b):
    return jnp.dot(a, b, preferred_element_type=jnp.float32)


def local(tokens, out_grad, gate_prob, routing, expert_weights):
    tok_dev, model_width = tokens.shape
    experts = lax.axis_size("expert")
    replicas = lax.axis_size("dp")
    chips = replicas // 2
    chip_bits = chips.bit_length() - 1
    capacity = 2 * tok_dev // experts
    share_rows = model_width // replicas
    half_rows = share_rows // 2
    grad_scale = float(tok_dev * replicas) ** (-0.5)
    weights = expert_weights[0]
    hidden_width = weights.shape[1] // 3
    pair_weights = weights[:, : 2 * hidden_width]
    down_weights = weights[:, 2 * hidden_width :]
    me = lax.axis_index("expert")
    replica = lax.axis_index("dp")
    core = replica % 2
    chip = replica // 2

    slot_index = slot_of(routing[:, 0], me, capacity, experts)
    table = (
        jnp.arange(experts * capacity, dtype=jnp.int32)[:, None] == slot_index[None, :]
    ).astype(jnp.bfloat16)

    def split(rows):
        return [rows[s * capacity : (s + 1) * capacity] for s in range(experts)]

    send_x = matmul(table, tokens).astype(jnp.bfloat16)
    recv_x = exchange(split(send_x), 1)
    scaled = (gate_prob * out_grad.astype(jnp.float32)).astype(jnp.bfloat16)
    send_g = matmul(table, scaled).astype(jnp.bfloat16)
    recv_g = exchange(split(send_g), 1)

    orders = [list(range(chip_bits)), list(range(chip_bits))[::-1]]
    ranks = [
        sorted(range(chips), key=lambda r: [-(r >> bit & 1) for bit in order]) for order in orders
    ]
    sends = [rank[: chips // 2] for rank in ranks]
    keeps = [rank[chips // 2 :] for rank in ranks]
    layout = [(r, h) for h in (0, 1) for r in sends[h]] + [(r, h) for h in (0, 1) for r in keeps[h]]

    def bands(rows, side):
        return jnp.concatenate(
            [
                lax.dynamic_slice_in_dim(
                    rows, ((chip ^ r) * 2 + side) * share_rows + h * half_rows, half_rows, 1
                )
                for r, h in layout
            ],
            axis=1,
        )

    def both_cores(rows):
        other = swap(bands(rows, 1 - core), 1, replicas)
        return jnp.concatenate([bands(rows, core), other], axis=0)

    rows_in = jnp.concatenate(recv_x, axis=0)
    pre_act = matmul(rows_in, pair_weights)
    wide_x = both_cores(rows_in)
    pre_gate = pre_act[:, :hidden_width]
    pre_up = pre_act[:, hidden_width:]
    sigmoid_gate = jax.nn.sigmoid(pre_gate)
    active = pre_gate * sigmoid_gate
    hidden = (active * pre_up).astype(jnp.bfloat16)
    slope = pre_up * (sigmoid_gate * (1.0 + pre_gate * (1.0 - sigmoid_gate)))
    wide_hidden = jnp.concatenate([hidden, swap(hidden, 1, replicas)], axis=0)

    recv_g, wide_x, wide_hidden, active, slope = lax.optimization_barrier(
        (recv_g, wide_x, wide_hidden, active, slope)
    )
    grad_in = jnp.concatenate(recv_g, axis=0)
    wide_g = both_cores(grad_in)
    grad_hidden = matmul(grad_in, down_weights)
    grad_gate = grad_hidden * slope
    grad_up = grad_hidden * active
    grad_pair = jnp.concatenate(
        [grad_gate.astype(jnp.bfloat16), grad_up.astype(jnp.bfloat16)], axis=1
    )
    returned = lax.dot_general(
        grad_pair, pair_weights, (((1,), (1,)), ((), ())), preferred_element_type=jnp.float32
    ).astype(jnp.bfloat16)
    arrived = exchange(split(returned), -1)

    wide_pair = jnp.concatenate([grad_pair, swap(grad_pair, 1, replicas)], axis=0)

    def block(start, count, wide_x, wide_g):
        cut = slice(start * half_rows, (start + count) * half_rows)
        first = lax.dot_general(wide_x[:, cut], wide_pair, ROWS, preferred_element_type=jnp.float32)
        second = lax.dot_general(
            wide_g[:, cut], wide_hidden, ROWS, preferred_element_type=jnp.float32
        )
        return grad_scale * jnp.concatenate([first, second], axis=1)

    def pieces(parts):
        rows = [p.shape[0] // half_rows for p in parts]
        return [
            p[i * half_rows : (i + 1) * half_rows] for p, n in zip(parts, rows) for i in range(n)
        ]

    count = chips // 2
    cuts = [(0, count // 2), (count // 2, count - count // 2)] if count > 1 else [(0, count)]
    came = [[], []]
    for start, length in cuts:
        parcels = [
            block(h * count + start, length, wide_x, wide_g).astype(jnp.bfloat16) for h in (0, 1)
        ]
        wide_x, wide_g, parcels = lax.optimization_barrier((wide_x, wide_g, parcels))
        for h in (0, 1):
            came[h].append(swap(parcels[h], 2 << orders[h][0], replicas))
    kept = [[], []]
    for start, length in cuts:
        for h in (0, 1):
            kept[h].append(block((2 + h) * count + start, length, wide_x, wide_g))
    values = [
        [
            k + c.astype(jnp.float32)
            for k, c in zip(pieces(kept[h]), pieces(came[h]))
        ]
        for h in (0, 1)
    ]
    for step in range(1, chip_bits):
        for h in (0, 1):
            bit = orders[h][step]
            half = len(values[h]) // 2
            out, stay = values[h][:half], values[h][half:]
            parcel = jnp.concatenate([v.astype(jnp.bfloat16) for v in out], axis=0)
            table, parcel = lax.optimization_barrier((table, parcel))
            got = swap(parcel, 2 << bit, replicas).astype(jnp.float32)
            values[h] = [v + g for v, g in zip(stay, pieces([got]))]
    totals = [values[0][0], values[1][0]]
    weight_grad = jnp.concatenate(totals, axis=0)

    input_grad = lax.dot_general(
        table, jnp.concatenate(arrived, axis=0), ROWS, preferred_element_type=jnp.float32
    ).astype(jnp.bfloat16)
    return (input_grad, weight_grad.reshape(1, share_rows, 3 * hidden_width))


def solution(mesh):
    in_specs = (
        P(("dp", "expert"), None),
        P(("dp", "expert"), None),
        P(("dp", "expert"), None),
        P(("dp", "expert"), None),
        P("expert", None, None),
    )
    out_specs = (P(("dp", "expert"), None), P("expert", "dp", None))
    return jax.shard_map(local, mesh=mesh, in_specs=in_specs, out_specs=out_specs, check_vma=False)
```

```python
import jax
import jax.numpy as jnp
from jax import lax
from jax.sharding import PartitionSpec as P


ROWS = (((0,), (0,)), ((), ()))


def slot_of(route_block, me, capacity, experts):
    relative = jnp.where(route_block >= me, route_block - me, route_block - me + experts)
    onehot = (relative[:, None] == jnp.arange(experts, dtype=jnp.int32)[None, :]).astype(jnp.int32)
    before = jnp.cumsum(onehot, axis=0) - onehot
    base = jnp.arange(experts, dtype=jnp.int32)[None, :] * capacity
    return jnp.sum((before + base) * onehot, axis=1)


def shift(value, distance, size):
    return lax.ppermute(value, "expert", [(j, (j + distance) % size) for j in range(size)])


def exchange(pieces, sign):
    size = len(pieces)
    moved = {0: pieces[0]}
    for distance in sorted(range(1, size), key=lambda s: -min(s, size - s)):
        moved[distance] = shift(pieces[distance], sign * distance, size)
    return [moved[s] for s in range(size)]


def swap(value, bit, size):
    return lax.ppermute(value, "dp", [(j, j ^ bit) for j in range(size)])


def matmul(a, b):
    return jnp.dot(a, b, preferred_element_type=jnp.float32)


def local(tokens, out_grad, gate_prob, routing, expert_weights):
    tok_dev, model_width = tokens.shape
    experts = lax.axis_size("expert")
    replicas = lax.axis_size("dp")
    chips = replicas // 2
    chip_bits = chips.bit_length() - 1
    capacity = 2 * tok_dev // experts
    share_rows = model_width // replicas
    half_rows = share_rows // 2
    grad_scale = float(tok_dev * replicas) ** (-0.5)
    weights = expert_weights[0]
    hidden_width = weights.shape[1] // 3
    pair_weights = weights[:, : 2 * hidden_width]
    down_weights = weights[:, 2 * hidden_width :]
    me = lax.axis_index("expert")
    replica = lax.axis_index("dp")
    core = replica % 2
    chip = replica // 2

    slot_index = slot_of(routing[:, 0], me, capacity, experts)
    table = (
        jnp.arange(experts * capacity, dtype=jnp.int32)[:, None] == slot_index[None, :]
    ).astype(jnp.bfloat16)

    def split(rows):
        return [rows[s * capacity : (s + 1) * capacity] for s in range(experts)]

    send_x = matmul(table, tokens).astype(jnp.bfloat16)
    recv_x = exchange(split(send_x), 1)
    scaled = (gate_prob * out_grad.astype(jnp.float32)).astype(jnp.bfloat16)
    send_g = matmul(table, scaled).astype(jnp.bfloat16)
    recv_g = exchange(split(send_g), 1)

    orders = [list(range(chip_bits)), list(range(chip_bits))[::-1]]
    ranks = [
        sorted(range(chips), key=lambda r: [-(r >> bit & 1) for bit in order]) for order in orders
    ]
    sends = [rank[: chips // 2] for rank in ranks]
    keeps = [rank[chips // 2 :] for rank in ranks]
    layout = [(r, h) for h in (0, 1) for r in sends[h]] + [(r, h) for h in (0, 1) for r in keeps[h]]

    def bands(rows, side):
        return jnp.concatenate(
            [
                lax.dynamic_slice_in_dim(
                    rows, ((chip ^ r) * 2 + side) * share_rows + h * half_rows, half_rows, 1
                )
                for r, h in layout
            ],
            axis=1,
        )

    def both_cores(rows):
        other = swap(bands(rows, 1 - core), 1, replicas)
        return jnp.concatenate([bands(rows, core), other], axis=0)

    rows_in = jnp.concatenate(recv_x, axis=0)
    pre_act = matmul(rows_in, pair_weights)
    wide_x = both_cores(rows_in)
    pre_gate = pre_act[:, :hidden_width]
    pre_up = pre_act[:, hidden_width:]
    sigmoid_gate = jax.nn.sigmoid(pre_gate)
    active = pre_gate * sigmoid_gate
    hidden = (active * pre_up).astype(jnp.bfloat16)
    slope = pre_up * (sigmoid_gate * (1.0 + pre_gate * (1.0 - sigmoid_gate)))
    wide_hidden = jnp.concatenate([hidden, swap(hidden, 1, replicas)], axis=0)

    recv_g, wide_x, wide_hidden, active, slope = lax.optimization_barrier(
        (recv_g, wide_x, wide_hidden, active, slope)
    )
    grad_in = jnp.concatenate(recv_g, axis=0)
    wide_g = both_cores(grad_in)
    grad_hidden = matmul(grad_in, down_weights)
    grad_gate = grad_hidden * slope
    grad_up = grad_hidden * active
    grad_pair = jnp.concatenate(
        [grad_gate.astype(jnp.bfloat16), grad_up.astype(jnp.bfloat16)], axis=1
    )
    returned = lax.dot_general(
        grad_pair, pair_weights, (((1,), (1,)), ((), ())), preferred_element_type=jnp.float32
    ).astype(jnp.bfloat16)
    arrived = exchange(split(returned), -1)

    wide_pair = jnp.concatenate([grad_pair, swap(grad_pair, 1, replicas)], axis=0)

    def block(start, count, wide_x, wide_g):
        cut = slice(start * half_rows, (start + count) * half_rows)
        first = lax.dot_general(wide_x[:, cut], wide_pair, ROWS, preferred_element_type=jnp.float32)
        second = lax.dot_general(
            wide_g[:, cut], wide_hidden, ROWS, preferred_element_type=jnp.float32
        )
        return grad_scale * jnp.concatenate([first, second], axis=1)

    def pieces(parts):
        rows = [p.shape[0] // half_rows for p in parts]
        return [
            p[i * half_rows : (i + 1) * half_rows] for p, n in zip(parts, rows) for i in range(n)
        ]

    count = chips // 2
    cuts = [(0, count // 2), (count // 2, count - count // 2)] if count > 1 else [(0, count)]
    came = [[], []]
    for start, length in cuts:
        parcels = [
            block(h * count + start, length, wide_x, wide_g).astype(jnp.bfloat16)
            for h in (0, 1)
        ]
        wide_x, wide_g, parcels = lax.optimization_barrier((wide_x, wide_g, parcels))
        for h in (0, 1):
            came[h].append(swap(parcels[h], 2 << orders[h][0], replicas))
    kept = [[], []]
    for start, length in cuts:
        for h in (0, 1):
            kept[h].append(block((2 + h) * count + start, length, wide_x, wide_g))
    values = [
        [
            k + c.astype(jnp.float32)
            for k, c in zip(pieces(kept[h]), pieces(came[h]))
        ]
        for h in (0, 1)
    ]
    for step in range(1, chip_bits):
        for h in (0, 1):
            bit = orders[h][step]
            half = len(values[h]) // 2
            out, stay = values[h][:half], values[h][half:]
            parcel = jnp.concatenate([v.astype(jnp.bfloat16) for v in out], axis=0)
            got = swap(parcel, 2 << bit, replicas).astype(jnp.float32)
            values[h] = [v + g for v, g in zip(stay, pieces([got]))]
    totals = [values[0][0], values[1][0]]
    weight_grad = jnp.concatenate(totals, axis=0)
    table, weight_grad = lax.optimization_barrier((table, weight_grad))

    input_grad = lax.dot_general(
        table, jnp.concatenate(arrived, axis=0), ROWS, preferred_element_type=jnp.float32
    ).astype(jnp.bfloat16)
    return (input_grad, weight_grad.reshape(1, share_rows, 3 * hidden_width))


def solution(mesh):
    in_specs = (
        P(("dp", "expert"), None),
        P(("dp", "expert"), None),
        P(("dp", "expert"), None),
        P(("dp", "expert"), None),
        P("expert", None, None),
    )
    out_specs = (P(("dp", "expert"), None), P("expert", "dp", None))

    return jax.shard_map(local, mesh=mesh, in_specs=in_specs, out_specs=out_specs, check_vma=False)
```
